32 devices in a mesh: row: 4 (over x, core), col: 8 (over z, y).
Axes of the slice: x: 2, y: 2, z: 4, core: 2. Of those that a mesh axis runs over, the one named last changes fastest.
Arguments:
- grid_tokens: bfloat16 [65536, 768], P(('row', 'col')), may hold values from -6 to 6
- grid_cotangent: bfloat16 [65536, 768], P(('row', 'col')), may hold values from -6 to 6
- send_rows: int32 [32, 512], P(('row', 'col')), may hold values from 0 to 2047, as said below
- send_counts: int32 [32, 32], P(('row', 'col')), may hold values from 1 to 16, as said below
- holder_segments: int32 [32, 512], P(('row', 'col')), may hold values from 0 to 3, as said below
- packed_master: float32 [768, 2304], P(('row', 'col')), may hold values from -0.21875 to 0.21875
- packed_first: float32 [768, 2304], P(('row', 'col')), may hold values from -80 to 80
- packed_second: float32 [768, 2304], P(('row', 'col')), may hold values from 430.8992 to 6897.664
- mixing_master: float32 [768, 768], P(('row', 'col')), may hold values from -1.75 to 1.75
- mixing_first: float32 [768, 768], P(('row', 'col')), may hold values from -12 to 12
- mixing_second: float32 [768, 768], P(('row', 'col')), may hold values from 9.66656 to 155.648
- expand_master: float32 [768, 3072], P(('row', 'col')), may hold values from -0.21875 to 0.21875
- expand_first: float32 [768, 3072], P(('row', 'col')), may hold values from -24 to 24
- expand_second: float32 [768, 3072], P(('row', 'col')), may hold values from 38.83008 to 620.9536
- reduce_master: float32 [3072, 768], P(('row', 'col')), may hold values from -0.109375 to 0.109375
- reduce_first: float32 [3072, 768], P(('row', 'col')), may hold values from -40 to 40
- reduce_second: float32 [3072, 768], P(('row', 'col')), may hold values from 107.80672 to 1720.32
- vector_master: float32 [12, 768], P(None, ('row', 'col')), may hold values from -1.2 to 1.3
- vector_first: float32 [12, 768], P(None, ('row', 'col')), may hold values from -128 to 128
- vector_second: float32 [12, 768], P(None, ('row', 'col')), may hold values from 969.9328 to 15515.648
Outputs:
- grid_output: bfloat16 [65536, 768], P(('row', 'col'))
- input_gradient: bfloat16 [65536, 768], P(('row', 'col'))
- packed_updated: float32 [768, 2304], P(('row', 'col'))
- packed_momentum: float32 [768, 2304], P(('row', 'col'))
- packed_variance: float32 [768, 2304], P(('row', 'col'))
- mixing_updated: float32 [768, 768], P(('row', 'col'))
- mixing_momentum: float32 [768, 768], P(('row', 'col'))
- mixing_variance: float32 [768, 768], P(('row', 'col'))
- expand_updated: float32 [768, 3072], P(('row', 'col'))
- expand_momentum: float32 [768, 3072], P(('row', 'col'))
- expand_variance: float32 [768, 3072], P(('row', 'col'))
- reduce_updated: float32 [3072, 768], P(('row', 'col'))
- reduce_momentum: float32 [3072, 768], P(('row', 'col'))
- reduce_variance: float32 [3072, 768], P(('row', 'col'))
- vector_updated: float32 [12, 768], P(None, ('row', 'col'))
- vector_momentum: float32 [12, 768], P(None, ('row', 'col'))
- vector_variance: float32 [12, 768], P(None, ('row', 'col'))
The draws below stay inside these ranges and needn't reach their ends.
Inputs may be any that keep to these rules, and one draw needn't show every extreme that they name: `send_rows`: entries holder * 16 to holder * 16 + 15 of a source's row list grid rows of that source for that holder; the first send_counts of them are live, and all live rows of one source are distinct; the rest name arbitrary rows. `send_counts`: some holder gets 16 live rows from every source. `holder_segments`: slot s * 16 + j of a holder carries an item number below 3 if j < send_counts[s, holder], else 3.
All inputs are finite; a program needn't handle non-finite values.
Results may differ from the reference program's by a relative error of at most 0.012.
The reference program's roundings to bfloat16 on the way count: a program that leaves them out, or rounds other values in their place, can miss the bound.
Values may be sent and summed in bfloat16 or wider, within the bound.
No kernel may reach another device: no remote copies, remote signals or barrier semaphores. Data moves between devices by JAX's collectives and lax.ppermute only.
A program may use at most 192 MiB of HBM per device.

```python
import math
import jax
import jax.numpy as jnp
from jax import lax

D = 768
HEADS = 12
HEAD_DIM = 64
FF = 3072
TOK_DEV = 2048
HOLD_DEV = 512
ITEMS_HOLD = 3
SLOT = 16
GRID_TOK = 65536
ROWS = 16384
VROWS = 12
DEVICES = 32


def routing_plan(key):
    root_key = jax.random.fold_in(key, 7)
    key_cap = jax.random.fold_in(root_key, 1)
    key_cut = jax.random.fold_in(root_key, 2)
    key_full = jax.random.fold_in(root_key, 3)
    key_perm = jax.random.fold_in(root_key, 4)
    key_item = jax.random.fold_in(root_key, 5)
    ceiling = jax.random.randint(key_cap, (DEVICES, 1), SLOT // 2, SLOT + 1)
    reduction = jax.random.randint(key_cut, (DEVICES, DEVICES), 0, SLOT // 4 + 1)
    counts = jnp.maximum(ceiling - reduction, 1)
    full_holder = jax.random.randint(key_full, (), 0, DEVICES)
    counts = jnp.where(jnp.arange(DEVICES)[None, :] == full_holder, SLOT, counts).astype(jnp.int32)
    orders = jax.vmap(lambda subkey: jax.random.permutation(subkey, TOK_DEV))(jax.random.split(key_perm, DEVICES))
    starts = jnp.cumsum(counts, axis=1) - counts
    places = (starts[:, :, None] + jnp.arange(SLOT)[None, None, :]).reshape(DEVICES, HOLD_DEV)
    send_list = jnp.take_along_axis(orders, places, axis=1).astype(jnp.int32)
    filled = jnp.arange(SLOT)[None, None, :] < counts.T[:, :, None]
    item_ids = jax.random.randint(key_item, (DEVICES, DEVICES, SLOT), 0, ITEMS_HOLD)
    segments = jnp.where(filled, item_ids, ITEMS_HOLD).reshape(DEVICES, HOLD_DEV).astype(jnp.int32)
    return (send_list, counts, segments)


def draw_send_rows(key, part):
    return routing_plan(key)[0]


def draw_send_counts(key, part):
    return routing_plan(key)[1]


def draw_holder_segments(key, part):
    return routing_plan(key)[2]


def draw_vector_master(key, part):
    noise = jax.random.normal(key, (VROWS, D), jnp.float32)
    uneven = jax.random.uniform(jax.random.fold_in(key, 1), (VROWS, D), jnp.float32, 0.7, 1.3)
    which_row = jnp.arange(VROWS)[:, None]
    is_gain = (which_row == 0) | (which_row == 5)
    return jnp.where(is_gain, uneven, 0.3 * jnp.clip(noise, -4.0, 4.0))


def level_of(key, shape, shards, least, top_value):
    loudness = 1.0
    for dim, blocks in shards:
        heights = jax.random.uniform(jax.random.fold_in(jax.random.fold_in(key, 6), dim), (blocks,), jnp.float32, least / len(shards), top_value / len(shards))
        loudness = loudness * jnp.repeat(jnp.exp(heights), shape[dim] // blocks).reshape((-1,) + (1,) * (len(shape) - 1 - dim))
    return loudness


def bell_draw(key, shape, scale, reach, cuts=(), kind=jnp.bfloat16):
    values = jax.random.normal(key, shape, jnp.float32) * scale
    if len(cuts) > 0:
        values = level_of(key, shape, cuts, -0.22, 0.18) * values
    return jnp.clip(values, min=-reach, max=reach).astype(kind)


def setup_inputs(seed: int = 0) -> dict:
    streams_of = jax.random.split(jax.random.key(seed), 21)
    grid_tokens = bell_draw(streams_of[0], (GRID_TOK, D), 1.0, 6.0, ((0, 32),))
    grid_cotangent = bell_draw(streams_of[1], (GRID_TOK, D), 1.0, 6.0, ((0, 32),))
    send_rows = draw_send_rows(jax.random.fold_in(streams_of[20], 71), 0)
    send_counts = draw_send_counts(jax.random.fold_in(streams_of[20], 71), 0)
    holder_segments = draw_holder_segments(jax.random.fold_in(streams_of[20], 71), 0)
    packed_master = bell_draw(streams_of[5], (D, 3 * D), D ** -0.5, 0.21875, ((0, 32),), jnp.float32)
    packed_first = bell_draw(streams_of[6], (D, 3 * D), (0.111 * ROWS ** 0.5), 80.0, ((0, 32),), jnp.float32)
    packed_second = jnp.clip(jnp.exp(math.log(6897.664) - 2.773064 * jax.random.uniform(streams_of[7], (D, 3 * D), jnp.float32) ** level_of(streams_of[7], (D, 3 * D), ((0, 32),), -0.2, 0.2)), 430.8992, 6897.664)
    mixing_master = bell_draw(streams_of[8], (D, D), (D // 64) ** -0.5, 1.75, ((0, 32),), jnp.float32)
    mixing_first = bell_draw(streams_of[9], (D, D), (0.0167 * ROWS ** 0.5), 12.0, ((0, 32),), jnp.float32)
    mixing_second = jnp.clip(jnp.exp(math.log(155.648) - 2.7789245 * jax.random.uniform(streams_of[10], (D, D), jnp.float32) ** level_of(streams_of[10], (D, D), ((0, 32),), -0.2, 0.2)), 9.66656, 155.648)
    expand_master = bell_draw(streams_of[11], (D, FF), D ** -0.5, 0.21875, ((0, 32),), jnp.float32)
    expand_first = bell_draw(streams_of[12], (D, FF), (0.0333 * ROWS ** 0.5), 24.0, ((0, 32),), jnp.float32)
    expand_second = jnp.clip(jnp.exp(math.log(620.9536) - 2.772061 * jax.random.uniform(streams_of[13], (D, FF), jnp.float32) ** level_of(streams_of[13], (D, FF), ((0, 32),), -0.2, 0.2)), 38.83008, 620.9536)
    reduce_master = bell_draw(streams_of[14], (FF, D), FF ** -0.5, 0.109375, ((0, 32),), jnp.float32)
    reduce_first = bell_draw(streams_of[15], (FF, D), (0.0556 * ROWS ** 0.5), 40.0, ((0, 32),), jnp.float32)
    reduce_second = jnp.clip(jnp.exp(math.log(1720.32) - 2.7699256 * jax.random.uniform(streams_of[16], (FF, D), jnp.float32) ** level_of(streams_of[16], (FF, D), ((0, 32),), -0.2, 0.2)), 107.80672, 1720.32)
    vector_master = draw_vector_master(jax.random.fold_in(streams_of[20], 71), 0)
    vector_first = bell_draw(streams_of[18], (VROWS, D), (0.167 * ROWS ** 0.5), 128.0, ((1, 32),), jnp.float32)
    vector_second = jnp.clip(jnp.exp(math.log(15515.648) - 2.7723776 * jax.random.uniform(streams_of[19], (VROWS, D), jnp.float32) ** level_of(streams_of[19], (VROWS, D), ((1, 32),), -0.2, 0.2)), 969.9328, 15515.648)
    return dict(grid_tokens=grid_tokens, grid_cotangent=grid_cotangent, send_rows=send_rows, send_counts=send_counts, holder_segments=holder_segments, packed_master=packed_master, packed_first=packed_first, packed_second=packed_second, mixing_master=mixing_master, mixing_first=mixing_first, mixing_second=mixing_second, expand_master=expand_master, expand_first=expand_first, expand_second=expand_second, reduce_master=reduce_master, reduce_first=reduce_first, reduce_second=reduce_second, vector_master=vector_master, vector_first=vector_first, vector_second=vector_second)


@jax.custom_vjp
def low(v):
    return lax.optimization_barrier(v.astype(jnp.bfloat16)).astype(jnp.float32)

@jax.custom_vjp
def low_back(v):
    return v

def low_keep(v):
    return (low(v), None)

def low_pass(kept, grad):
    return (grad,)

def back_keep(v):
    return (v, None)

def back_low(kept, grad):
    return (low(grad),)
low.defvjp(low_keep, low_pass)
low_back.defvjp(back_keep, back_low)
weight_rates = (0.07, 0.55, 0.07, 0.036, 0.4)
decay_rates = (0.05, 0.05, 0.05, 0.05, 0.0)

def matmul(left, right):
    return jnp.dot(left, right, precision=lax.Precision.HIGHEST, preferred_element_type=jnp.float32)

def normalize(values):
    center = values - lax.optimization_barrier(jnp.mean(values, axis=-1, keepdims=True))
    spread = lax.optimization_barrier(jnp.mean(center * center, axis=-1, keepdims=True))
    return center * lax.rsqrt(spread + 1e-06)

def attend(queries, keys_all, values_all, segments):
    span_rows = min(512, HOLD_DEV)
    count_blocks = HOLD_DEV // span_rows
    scaling = HEAD_DIM ** (-0.5)
    query_blocks = queries.reshape(count_blocks, span_rows, HEADS, HEAD_DIM)
    segment_blocks = segments.reshape(count_blocks, span_rows)

    def one_block(pieces):
        query_part, segment_part = pieces
        scores = jnp.einsum('qhd,khd->hqk', query_part, keys_all, precision=lax.Precision.HIGHEST) * scaling
        scores = low_back(scores)
        allowed = (segment_part[:, None] == segments[None, :])[None]
        scores = jnp.where(allowed, scores, -1e+30)
        highest = lax.optimization_barrier(jnp.max(scores, axis=-1, keepdims=True))
        weights = jnp.exp(scores - highest)
        shares = low(weights / lax.optimization_barrier(jnp.sum(weights, axis=-1, keepdims=True)))
        return jnp.einsum('hqk,khd->qhd', shares, values_all, precision=lax.Precision.HIGHEST)
    mixed = lax.map(jax.checkpoint(one_block), (query_blocks, segment_blocks))
    return mixed.reshape(HOLD_DEV, HEADS * HEAD_DIM)

def layer(inputs, w_packed, w_mixing, w_expand, w_reduce, vectors, segments):
    features = inputs.shape[1]
    gain_one = vectors[0]
    shift_one = vectors[1]
    bias_query = vectors[2]
    bias_value = vectors[3]
    bias_mixing = vectors[4]
    gain_two = vectors[5]
    shift_two = vectors[6]
    bias_output = vectors[7]
    bias_hidden = vectors[8:].reshape(-1)
    layer_one = low(normalize(inputs) * gain_one + shift_one)
    joined_bias = jnp.concatenate([bias_query, jnp.zeros_like(bias_query), bias_value])
    project = low_back(low(matmul(layer_one, w_packed) + joined_bias))
    queries = project[:, :features].reshape(-1, HEADS, HEAD_DIM)
    keys_all = project[:, features:2 * features].reshape(-1, HEADS, HEAD_DIM)
    values_all = project[:, 2 * features:].reshape(-1, HEADS, HEAD_DIM)
    attended = low_back(low(attend(queries, keys_all, values_all, segments)))
    branch_one = low_back(matmul(attended, w_mixing) + bias_mixing)
    middle = inputs + branch_one
    layer_two = low(normalize(middle) * gain_two + shift_two)
    hidden_pre = low_back(matmul(layer_two, w_expand) + bias_hidden)
    hidden_act = low(jax.nn.gelu(hidden_pre, approximate=False))
    branch_two = low_back(matmul(hidden_act, w_reduce) + bias_output)
    return middle + branch_two

def adamw(master, moment_one, moment_two, gradient, step_rate, decay_rate):
    first_new = 0.9 * moment_one + 0.1 * gradient
    second_new = 0.95 * moment_two + 0.05 * gradient * gradient
    moved = first_new / (1.0 - 0.9 ** 10) / (jnp.sqrt(second_new / (1.0 - 0.95 ** 10)) + 1e-08)
    return (master - step_rate * (moved + decay_rate * master), first_new, second_new)

def reference(grid_tokens, grid_cotangent, send_rows, send_counts, holder_segments, packed_master, packed_first, packed_second, mixing_master, mixing_first, mixing_second, expand_master, expand_first, expand_second, reduce_master, reduce_first, reduce_second, vector_master, vector_first, vector_second):
    masters = (packed_master, mixing_master, expand_master, reduce_master, vector_master)
    firsts = (packed_first, mixing_first, expand_first, reduce_first, vector_first)
    seconds = (packed_second, mixing_second, expand_second, reduce_second, vector_second)
    copies = tuple((master.astype(jnp.bfloat16).astype(jnp.float32) for master in masters))
    tokens = grid_tokens.astype(jnp.float32)
    cotangent = grid_cotangent.astype(jnp.float32)
    slot_place = jnp.arange(SLOT, dtype=jnp.int32)
    source_base = jnp.arange(DEVICES, dtype=jnp.int32)[:, None] * TOK_DEV
    zero_totals = tuple((jnp.zeros_like(copy_one) for copy_one in copies))

    def holder_step(totals, holder):
        columns = lax.dynamic_slice_in_dim(send_rows, holder * SLOT, SLOT, 1)
        counted = lax.dynamic_slice_in_dim(send_counts, holder, 1, 1)
        live_rows = (slot_place[None, :] < counted).reshape(-1, 1).astype(jnp.float32)
        row_index = (columns + source_base).reshape(-1).astype(jnp.int32)
        gathered = tokens[row_index] * live_rows
        returned = cotangent[row_index] * live_rows
        segments = holder_segments[holder]

        def forward(inputs, w_packed, w_mixing, w_expand, w_reduce, vectors):
            return layer(inputs, w_packed, w_mixing, w_expand, w_reduce, vectors, segments)
        outputs, pullback = jax.vjp(forward, gathered, *copies)
        gradients = pullback(returned)
        totals = tuple((total + gradient for total, gradient in zip(totals, gradients[1:])))
        return (totals, (outputs.astype(jnp.bfloat16), gradients[0].astype(jnp.bfloat16)))
    summed, (held_out, held_grad) = lax.scan(holder_step, zero_totals, jnp.arange(DEVICES, dtype=jnp.int32))
    all_columns = send_rows.reshape(DEVICES, DEVICES, SLOT).transpose(1, 0, 2) + source_base[None]
    all_live = (slot_place[None, None, :] < send_counts.T[:, :, None]).astype(jnp.float32).reshape(-1, 1)
    flat_index = all_columns.reshape(-1).astype(jnp.int32)
    grid_output = jnp.zeros((GRID_TOK, D), jnp.float32).at[flat_index].add(held_out.reshape(-1, D).astype(jnp.float32) * all_live).astype(jnp.bfloat16)
    input_gradient = jnp.zeros((GRID_TOK, D), jnp.float32).at[flat_index].add(held_grad.reshape(-1, D).astype(jnp.float32) * all_live).astype(jnp.bfloat16)
    updates = [adamw(masters[number], firsts[number], seconds[number], summed[number], weight_rates[number], decay_rates[number]) for number in range(5)]
    return (grid_output, input_gradient, updates[0][0], updates[0][1], updates[0][2], updates[1][0], updates[1][1], updates[1][2], updates[2][0], updates[2][1], updates[2][2], updates[3][0], updates[3][1], updates[3][2], updates[4][0], updates[4][1], updates[4][2])
```

```python
import jax
import jax.numpy as jnp
from jax import lax
from jax.sharding import PartitionSpec as P

HEADS = 12
HEAD_DIM = 64


weight_rates = (0.07, 0.55, 0.07, 0.036, 0.4)
decay_rates = (0.05, 0.05, 0.05, 0.05, 0.0)


def normalize(values):
    center = values - jnp.mean(values, axis=-1, keepdims=True)
    spread = jnp.mean(center * center, axis=-1, keepdims=True)
    factor = lax.rsqrt(spread + 1e-06)
    return (center * factor, factor)


def norm_back(upstream, normed, factor, gain):
    scaled = upstream * gain
    return factor * (
        scaled
        - jnp.mean(scaled, axis=-1, keepdims=True)
        - normed * jnp.mean(scaled * normed, axis=-1, keepdims=True)
    )


def gelu_slope(values):
    cumulative = 0.5 * (1.0 + lax.erf(values * 0.7071067811865476))
    return cumulative + values * jnp.exp(-0.5 * values * values) * 0.3989422804014327


def masked_scores(query_part, keys_all, segment_part, segments):
    scores = jnp.einsum(
        "qhd,khd->hqk", query_part, keys_all, preferred_element_type=jnp.float32
    ) * HEAD_DIM ** (-0.5)
    allowed = (segment_part[:, None] == segments[None, :])[None]
    return jnp.where(allowed, scores, -1e30)


def adamw(master, moment_one, moment_two, gradient, step_rate, decay_rate):
    first_new = 0.9 * moment_one + 0.1 * gradient
    second_new = 0.95 * moment_two + 0.05 * gradient * gradient
    moved = first_new / (1.0 - 0.9**10) / (jnp.sqrt(second_new / (1.0 - 0.95**10)) + 1e-08)
    return (master - step_rate * (moved + decay_rate * master), first_new, second_new)


def holder_pass(arrived, arrived_grad, segments, w_packed, w_mixing, w_expand, w_reduce, vectors):
    total_rows, features = arrived.shape
    inputs = arrived.astype(jnp.float32)
    gain_one = vectors[0]
    shift_one = vectors[1]
    bias_query = vectors[2]
    bias_value = vectors[3]
    bias_mixing = vectors[4]
    gain_two = vectors[5]
    shift_two = vectors[6]
    bias_output = vectors[7]
    bias_hidden = vectors[8:].reshape(-1)
    normed_one, factor_one = normalize(inputs)
    layer_one = (normed_one * gain_one + shift_one).astype(jnp.bfloat16)
    joined_bias = jnp.concatenate([bias_query, jnp.zeros_like(bias_query), bias_value])
    project = (
        jnp.dot(layer_one, w_packed, preferred_element_type=jnp.float32) + joined_bias
    ).astype(jnp.bfloat16)
    queries = project[:, :features].reshape(total_rows, HEADS, HEAD_DIM)
    keys_all = project[:, features : 2 * features].reshape(total_rows, HEADS, HEAD_DIM)
    values_all = project[:, 2 * features :].reshape(total_rows, HEADS, HEAD_DIM)
    span_rows = min(512, total_rows)
    offsets = list(range(0, total_rows, span_rows))
    mixed_parts = []
    log_totals = []
    for offset in offsets:
        scores = masked_scores(queries, keys_all, segments, segments)
        highest = jnp.max(scores, axis=-1)
        weights = jnp.exp(scores - highest[..., None])
        totals = jnp.sum(weights, axis=-1)
        shares = (weights / totals[..., None]).astype(jnp.bfloat16)
        mixed_parts.append(
            jnp.einsum("hqk,khd->qhd", shares, values_all, preferred_element_type=jnp.float32)
        )
        log_totals.append(highest + jnp.log(totals))
    attended = mixed_parts[0].reshape(total_rows, features).astype(jnp.bfloat16)
    middle = inputs + jnp.dot(attended, w_mixing, preferred_element_type=jnp.float32) + bias_mixing
    normed_two, factor_two = normalize(middle)
    layer_two = (normed_two * gain_two + shift_two).astype(jnp.bfloat16)
    hidden_pre = jnp.dot(layer_two, w_expand, preferred_element_type=jnp.float32) + bias_hidden
    hidden_act = jax.nn.gelu(hidden_pre, approximate=False).astype(jnp.bfloat16)
    outputs = (
        middle + jnp.dot(hidden_act, w_reduce, preferred_element_type=jnp.float32) + bias_output
    )
    upstream = arrived_grad.astype(jnp.float32)
    d_hidden = (
        jnp.dot(arrived_grad, w_reduce.T, preferred_element_type=jnp.float32)
        * gelu_slope(hidden_pre)
    ).astype(jnp.bfloat16)
    d_layer_two = jnp.dot(d_hidden, w_expand.T, preferred_element_type=jnp.float32)
    d_middle = upstream + norm_back(d_layer_two, normed_two, factor_two, gain_two)
    d_branch = d_middle.astype(jnp.bfloat16)
    d_attended = (
        jnp.dot(d_branch, w_mixing.T, preferred_element_type=jnp.float32)
        .astype(jnp.bfloat16)
        .reshape(total_rows, HEADS, HEAD_DIM)
    )
    d_keys = jnp.zeros((total_rows, HEADS, HEAD_DIM), jnp.float32)
    d_values = jnp.zeros((total_rows, HEADS, HEAD_DIM), jnp.float32)
    d_query_parts = []
    for number, offset in enumerate(offsets):
        scores = masked_scores(queries, keys_all, segments, segments)
        chances = jnp.exp(scores - log_totals[number][..., None])
        d_chances = jnp.einsum(
            "qhd,khd->hqk", d_attended, values_all, preferred_element_type=jnp.float32
        )
        d_values = jnp.einsum(
            "hqk,qhd->khd",
            chances.astype(jnp.bfloat16),
            d_attended,
            preferred_element_type=jnp.float32,
        )
        row_dot = jnp.sum(chances * d_chances, axis=-1, keepdims=True)
        d_scores = (chances * (d_chances - row_dot)).astype(jnp.bfloat16)
        d_query_parts.append(
            jnp.einsum("hqk,khd->qhd", d_scores, keys_all, preferred_element_type=jnp.float32)
            * HEAD_DIM ** (-0.5)
        )
        d_keys = jnp.einsum("hqk,qhd->khd", d_scores, queries, preferred_element_type=jnp.float32)
    d_project = jnp.concatenate(
        [
            d_query_parts[0].reshape(total_rows, features),
            (d_keys * HEAD_DIM ** (-0.5)).reshape(total_rows, features),
            d_values.reshape(total_rows, features),
        ],
        axis=1,
    ).astype(jnp.bfloat16)
    d_layer_one = jnp.dot(d_project, w_packed.T, preferred_element_type=jnp.float32)
    input_grads = d_middle + norm_back(d_layer_one, normed_one, factor_one, gain_one)
    vector_rows = jnp.stack(
        [
            jnp.sum(d_layer_one * normed_one, axis=0),
            jnp.sum(d_layer_one, axis=0),
            jnp.sum(d_project[:, :features], axis=0, dtype=jnp.float32),
            jnp.sum(d_project[:, 2 * features :], axis=0, dtype=jnp.float32),
            jnp.sum(d_branch, axis=0, dtype=jnp.float32),
            jnp.sum(d_layer_two * normed_two, axis=0),
            jnp.sum(d_layer_two, axis=0),
            jnp.sum(upstream, axis=0),
        ]
    )
    grad_vector = jnp.concatenate(
        [vector_rows, jnp.sum(d_hidden, axis=0, dtype=jnp.float32).reshape(-1, features)], axis=0
    )
    return (
        outputs.astype(jnp.bfloat16),
        input_grads.astype(jnp.bfloat16),
        (
            (layer_one, d_project),
            (attended, d_branch),
            (layer_two, d_hidden),
            (hidden_act, arrived_grad),
            grad_vector,
        ),
    )


AXES = ("row", "col")


def swap(values, bit):
    devices = lax.axis_size(AXES)
    return lax.ppermute(values, AXES, [(d, d ^ (1 << bit)) for d in range(devices)])


def bit_orders():
    rows, cols = lax.axis_size("row"), lax.axis_size("col")
    low_bits = cols.bit_length() - 1
    all_bits = (rows * cols).bit_length() - 1
    core, high, low = low_bits, list(range(low_bits + 1, all_bits)), list(range(low_bits))
    return ([core] + high + low, [core] + low[:1] + high + low[1:])


def relative(blocks):
    devices = blocks.shape[0]
    order = jnp.arange(devices, dtype=jnp.int32) ^ lax.axis_index(AXES)
    return jnp.take(blocks, order, axis=0, mode="clip")


def split_bit(values, bits, bit):
    place = bits.index(bit)
    return (
        lax.index_in_dim(values, 0, place, keepdims=False),
        lax.index_in_dim(values, 1, place, keepdims=False),
    )


def reduce_halves(keep, send, bits, order, kind):
    bits = [b for b in bits if b != order[0]]
    got = swap(send, order[0])
    for bit in order[1:]:
        keep_low, keep_high = split_bit(keep, bits, bit)
        got_low, got_high = split_bit(got, bits, bit)
        send = (keep_high.astype(jnp.float32) + got_high.astype(jnp.float32)).astype(kind)
        keep = (keep_low.astype(jnp.float32) + got_low.astype(jnp.float32)).astype(kind)
        bits = [b for b in bits if b != bit]
        got = swap(send, bit)
    return keep.astype(jnp.float32) + got.astype(jnp.float32)


def weight_gradient(left, right, orders):
    devices = lax.axis_size(AXES)
    count = devices.bit_length() - 1
    bits = list(range(count - 1, -1, -1))
    tokens, features = left.shape
    rows = features // devices
    turned = relative(left.T.reshape(devices, rows, tokens)).reshape([2] * count + [rows, tokens])
    keep_rows, send_rows = split_bit(turned, bits, orders[0][0])
    width = right.shape[1] // len(orders)
    parts = []
    for number, order in enumerate(orders):
        chunk = right[:, number * width : (number + 1) * width]

        def product(side):
            flat = side.reshape(-1, tokens)
            out = jnp.dot(flat, chunk, preferred_element_type=jnp.float32).astype(jnp.bfloat16)
            return out.reshape([2] * (count - 1) + [rows, width])

        parts.append(
            reduce_halves(product(keep_rows), product(send_rows), bits, order, jnp.bfloat16)
        )
    return parts[0] if len(parts) == 1 else jnp.concatenate(parts, axis=1)


def vector_gradient(gradient, order):
    devices = lax.axis_size(AXES)
    count = devices.bit_length() - 1
    bits = list(range(count - 1, -1, -1))
    lines, features = gradient.shape
    blocks = relative(gradient.reshape(lines, devices, features // devices).transpose(1, 0, 2))
    blocks = blocks.reshape([2] * count + [lines, features // devices])
    keep, send = split_bit(blocks, bits, order[0])
    return reduce_halves(keep, send, bits, order, jnp.float32)


def gather_blocks(shard, order):
    devices = lax.axis_size(AXES)
    count = devices.bit_length() - 1
    held = shard[None]
    for bit in reversed(order):
        held = jnp.concatenate([held, swap(held, bit)], axis=0)
    ranks = jnp.arange(devices, dtype=jnp.int32) ^ lax.axis_index(AXES)
    place = jnp.zeros_like(ranks)
    for step, bit in enumerate(reversed(order)):
        place = place | (((ranks >> bit) & 1) << step)
    return jnp.take(held, place, axis=0, mode="clip")


def gather_rows(shard, orders):
    devices = lax.axis_size(AXES)
    width = shard.shape[1] // len(orders)
    parts = []
    for number, order in enumerate(orders):
        blocks = gather_blocks(shard[:, number * width : (number + 1) * width], order)
        parts.append(blocks.reshape(devices * shard.shape[0], width))
    return parts[0] if len(parts) == 1 else jnp.concatenate(parts, axis=1)


def on_device(
    grid_tokens,
    grid_cotangent,
    send_rows,
    send_counts,
    holder_segments,
    packed_master,
    packed_first,
    packed_second,
    mixing_master,
    mixing_first,
    mixing_second,
    expand_master,
    expand_first,
    expand_second,
    reduce_master,
    reduce_first,
    reduce_second,
    vector_master,
    vector_first,
    vector_second,
):
    devices = lax.axis_size(AXES)
    holding = send_rows.shape[1]
    slot_rows = holding // devices
    tokens, features = grid_tokens.shape
    first, second = bit_orders()
    w_packed = gather_rows(packed_master.astype(jnp.bfloat16), [first, second])
    w_mixing = gather_rows(mixing_master.astype(jnp.bfloat16), [first])
    w_expand = gather_rows(expand_master.astype(jnp.bfloat16), [second])
    w_reduce = gather_rows(reduce_master.astype(jnp.bfloat16), [first])
    vector_low = gather_blocks(vector_master.astype(jnp.bfloat16), second)
    vector_low = vector_low.transpose(1, 0, 2).reshape(vector_master.shape[0], features)
    slots = jnp.arange(slot_rows, dtype=jnp.int32)[None, :]
    live = (slots < send_counts[0][:, None]).reshape(holding)
    row_index = jnp.where(live, send_rows[0], -1)
    pick = (row_index[:, None] == jnp.arange(tokens, dtype=jnp.int32)[None, :]).astype(jnp.bfloat16)

    def send(rows):
        blocks = rows.reshape(devices, slot_rows, features)
        moved = lax.all_to_all(blocks, AXES, split_axis=0, concat_axis=0, tiled=True)
        return moved.reshape(holding, features)

    def take_rows(grid):
        return jnp.dot(pick, grid, preferred_element_type=jnp.float32).astype(jnp.bfloat16)

    def put_rows(rows):
        return lax.dot_general(
            pick, rows, (((0,), (0,)), ((), ())), preferred_element_type=jnp.float32
        ).astype(jnp.bfloat16)

    results, input_grads, pairs = holder_pass(
        send(take_rows(grid_tokens)),
        send(take_rows(grid_cotangent)),
        holder_segments[0],
        w_packed,
        w_mixing,
        w_expand,
        w_reduce,
        vector_low.astype(jnp.float32),
    )
    grid_output = put_rows(send(results))
    input_gradient = put_rows(send(input_grads))
    masters = (packed_master, mixing_master, expand_master, reduce_master, vector_master)
    firsts = (packed_first, mixing_first, expand_first, reduce_first, vector_first)
    seconds = (packed_second, mixing_second, expand_second, reduce_second, vector_second)
    shares = (
        weight_gradient(*pairs[0], [first, second]),
        weight_gradient(*pairs[1], [first]),
        weight_gradient(*pairs[2], [second]),
        weight_gradient(*pairs[3], [first]),
        vector_gradient(pairs[4], second),
    )
    updates = [
        adamw(
            masters[number],
            firsts[number],
            seconds[number],
            shares[number],
            weight_rates[number],
            decay_rates[number],
        )
        for number in range(5)
    ]
    return (
        grid_output,
        input_gradient,
        updates[0][0],
        updates[0][1],
        updates[0][2],
        updates[1][0],
        updates[1][1],
        updates[1][2],
        updates[2][0],
        updates[2][1],
        updates[2][2],
        updates[3][0],
        updates[3][1],
        updates[3][2],
        updates[4][0],
        updates[4][1],
        updates[4][2],
    )


def solution(mesh):
    in_specs = (
        P(("row", "col"), None),
        P(("row", "col"), None),
        P(("row", "col"), None),
        P(("row", "col"), None),
        P(("row", "col"), None),
        P(("row", "col"), None),
        P(("row", "col"), None),
        P(("row", "col"), None),
        P(("row", "col"), None),
        P(("row", "col"), None),
        P(("row", "col"), None),
        P(("row", "col"), None),
        P(("row", "col"), None),
        P(("row", "col"), None),
        P(("row", "col"), None),
        P(("row", "col"), None),
        P(("row", "col"), None),
        P(None, ("row", "col")),
        P(None, ("row", "col")),
        P(None, ("row", "col")),
    )
    out_specs = (
        P(("row", "col"), None),
        P(("row", "col"), None),
        P(("row", "col"), None),
        P(("row", "col"), None),
        P(("row", "col"), None),
        P(("row", "col"), None),
        P(("row", "col"), None),
        P(("row", "col"), None),
        P(("row", "col"), None),
        P(("row", "col"), None),
        P(("row", "col"), None),
        P(("row", "col"), None),
        P(("row", "col"), None),
        P(("row", "col"), None),
        P(None, ("row", "col")),
        P(None, ("row", "col")),
        P(None, ("row", "col")),
    )
    return jax.shard_map(
        on_device, mesh=mesh, in_specs=in_specs, out_specs=out_specs, check_vma=False
    )
```

```python
import jax
import jax.numpy as jnp
from jax import lax
from jax.experimental import pallas as pl
from jax.experimental.pallas import tpu as pltpu
from jax.sharding import PartitionSpec as P

HEAD_DIM = 64


weight_rates = (0.07, 0.55, 0.07, 0.036, 0.4)
decay_rates = (0.05, 0.05, 0.05, 0.05, 0.0)


def normalize(values):
    center = values - jnp.mean(values, axis=-1, keepdims=True)
    spread = jnp.mean(center * center, axis=-1, keepdims=True)
    factor = lax.rsqrt(spread + 1e-06)
    return (center * factor, factor)


def norm_back(upstream, normed, factor, gain):
    scaled = upstream * gain
    return factor * (
        scaled
        - jnp.mean(scaled, axis=-1, keepdims=True)
        - normed * jnp.mean(scaled * normed, axis=-1, keepdims=True)
    )


def adamw(master, moment_one, moment_two, gradient, step_rate, decay_rate):
    first_new = 0.9 * moment_one + 0.1 * gradient
    second_new = 0.95 * moment_two + 0.05 * gradient * gradient
    moved = first_new / (1.0 - 0.9**10) / (jnp.sqrt(second_new / (1.0 - 0.95**10)) + 1e-08)
    return (master - step_rate * (moved + decay_rate * master), first_new, second_new)


AXES = ("row", "col")
HIDDEN_BLOCK = 768
TOKEN_BLOCK = 256
f32 = jnp.float32
bf16 = jnp.bfloat16


def dot(left, right, dims=((1,), (0,))):
    return lax.dot_general(left, right, (dims, ((), ())), preferred_element_type=f32)


def swap(values, bit):
    devices = lax.axis_size(AXES)
    return lax.ppermute(values, AXES, [(d, d ^ (1 << bit)) for d in range(devices)])


def bit_orders():
    rows, cols = lax.axis_size("row"), lax.axis_size("col")
    low_bits = cols.bit_length() - 1
    all_bits = (rows * cols).bit_length() - 1
    core, high, low = low_bits, list(range(low_bits + 1, all_bits)), list(range(low_bits))
    return ([core] + high + low, [core] + low[:1] + high + low[1:])


def place_of(order):
    count = len(order)
    return [
        sum(((r >> bit) & 1) << (count - 1 - step) for step, bit in enumerate(order))
        for r in range(1 << count)
    ]


def block_places(order):
    table = jnp.asarray(place_of(order), jnp.int32)
    ranks = jnp.arange(len(table), dtype=jnp.int32) ^ lax.axis_index(AXES)
    return jnp.take(table, ranks, mode="clip")


def by_place(blocks, order):
    table = place_of(order)
    back = [table.index(p) for p in range(len(table))]
    ranks = jnp.asarray(back, jnp.int32) ^ lax.axis_index(AXES)
    return jnp.take(blocks, ranks, axis=0, mode="clip")


class Chain:
    def __init__(self, keep, send, order, kind=bf16):
        self.keep, self.send, self.order, self.kind = keep, send, list(order), kind
        self.launch()

    def launch(self):
        self.got = swap(self.send, self.order.pop(0))

    def merge(self):
        half = self.keep.shape[0] // 2
        keep, got = self.keep, self.got
        self.send = (keep[half:].astype(f32) + got[half:].astype(f32)).astype(self.kind)
        self.keep = (keep[:half].astype(f32) + got[:half].astype(f32)).astype(self.kind)

    def total(self):
        return (self.keep.astype(f32) + self.got.astype(f32))[0]


def turn(values, chains):
    values, gots = lax.optimization_barrier((values, [c.got for c in chains]))
    for chain, got in zip(chains, gots):
        chain.got = got
        chain.merge()
    values, sends = lax.optimization_barrier((values, [c.send for c in chains]))
    for chain, part in zip(chains, sends):
        chain.send = part
        chain.launch()
    return values


def halves(blocks):
    half = blocks.shape[0] // 2
    return blocks[:half], blocks[half:]


def weight_chain(pairs, order):
    devices = lax.axis_size(AXES)
    keeps, sends = [], []
    for left, right in pairs:
        tokens, features = left.shape
        rows = features // devices
        turned = by_place(left.T.reshape(devices, rows, tokens), order)
        for side, parts in zip(halves(turned), (keeps, sends)):
            flat = dot(side.reshape(-1, tokens), right).astype(bf16)
            parts.append(flat.reshape(-1, rows, right.shape[1]))
    join = lambda parts: parts[0] if len(parts) == 1 else jnp.concatenate(parts, axis=-1)
    return Chain(join(keeps), join(sends), order)


class Gather:
    def __init__(self, shard, order):
        self.order, self.held, self.left = order, shard[None], list(reversed(order))
        self.launch()

    def launch(self):
        self.got = swap(self.held, self.left.pop(0))

    def merge(self):
        self.held = jnp.concatenate([self.held, self.got], axis=0)

    def blocks(self):
        self.merge()
        return jnp.take(self.held, block_places(self.order), axis=0, mode="clip")


def gather_turn(values, gathers):
    values, gots = lax.optimization_barrier((values, [g.got for g in gathers]))
    for gather, got in zip(gathers, gots):
        gather.got = got
        gather.merge()
    values, helds = lax.optimization_barrier((values, [g.held for g in gathers]))
    for gather, held in zip(gathers, helds):
        gather.held = held
        gather.launch()
    return values


def mlp_kernel(
    place_r, place_e, a2, dy, we, wr, bias,
    out_y, out_da, keep_r, send_r, keep_e, send_e, out_gb, u_all, dz_all, we_all,
):
    step = pl.program_id(0)
    tokens, features = a2.shape
    half = keep_r.shape[0]

    @pl.when(step == 0)
    def _():
        out_y[...] = jnp.zeros_like(out_y)
        out_da[...] = jnp.zeros_like(out_da)

    if len(we.shape) == 2:
        we_all[...] = we[...]
    else:
        rows_e = we.shape[1]
        for s in range(we.shape[0]):
            we_all[s * rows_e : (s + 1) * rows_e, :] = we[s]
    wr_all = wr[...].reshape(HIDDEN_BLOCK, features)

    def chunk(number, total):
        rows = pl.ds(pl.multiple_of(number * TOKEN_BLOCK, TOKEN_BLOCK), TOKEN_BLOCK)
        z = dot(a2[rows, :], we_all[...]) + bias[...]
        cumulative = 0.5 * (1.0 + lax.erf(z * 0.7071067811865476))
        u = (z * cumulative).astype(bf16)
        slope = cumulative + z * jnp.exp(-0.5 * z * z) * 0.3989422804014327
        dz = (dot(dy[rows, :], wr_all, ((1,), (1,))) * slope).astype(bf16)
        u_all[rows, :] = u
        dz_all[rows, :] = dz
        out_y[rows, :] += dot(u, wr_all)
        out_da[rows, :] += dot(dz, we_all[...], ((1,), (1,)))
        return total + jnp.sum(dz.astype(f32), axis=0, keepdims=True)

    out_gb[...] = lax.fori_loop(0, tokens // TOKEN_BLOCK, chunk, jnp.zeros(out_gb.shape, f32))

    def store(place, block, keep, send):
        @pl.when(place < half)
        def _():
            keep[place] = block

        @pl.when(place >= half)
        def _():
            send[place - half] = block

    rows_r = keep_r.shape[1]
    per_step = HIDDEN_BLOCK // rows_r
    grad = dot(u_all[...], dy[...], ((0,), (0,))).astype(bf16)
    for j in range(per_step):
        store(place_r[step * per_step + j], grad[j * rows_r : (j + 1) * rows_r], keep_r, send_r)
    grad = dot(a2[...], dz_all[...], ((0,), (0,))).astype(bf16)
    if len(keep_e.shape) == 2:
        keep_e[...] = grad
    else:
        rows_e = keep_e.shape[1]
        for s in range(2 * half):
            store(place_e[s], grad[s * rows_e : (s + 1) * rows_e], keep_e, send_e)


def mlp(a2, dy, both, bias, order_r, order_e):
    devices = lax.axis_size(AXES)
    tokens, features = a2.shape
    rows_r = both.shape[1] // 2
    hidden = devices * rows_r
    rows_e, wide = features // devices, hidden // features
    half = devices // 2
    direct = rows_e % 8 == 0
    whole = lambda *shape: pl.BlockSpec(shape, lambda i, *_: (0,) * len(shape))
    columns = pl.BlockSpec((features, HIDDEN_BLOCK), lambda i, *_: (0, i))
    if direct:
        we = both.reshape(devices, 2 * wide, rows_e, features)
        spec_we = pl.BlockSpec((devices, None, rows_e, features), lambda i, *_: (0, i, 0, 0))
        spec_e = [pl.BlockSpec((half, rows_e, HIDDEN_BLOCK), lambda i, *_: (0, 0, i))] * 2
        shape_e = [(half, rows_e, hidden)] * 2
    else:
        we = both[:, :rows_r].reshape(devices, wide, rows_e, features)
        we = we.transpose(0, 2, 1, 3).reshape(features, hidden)
        spec_we = columns
        spec_e = [columns, pl.BlockSpec((8, HIDDEN_BLOCK), lambda i, *_: (0, i))]
        shape_e = [(features, hidden), (8, hidden)]
    per_step = HIDDEN_BLOCK // rows_r
    grid_spec = pltpu.PrefetchScalarGridSpec(
        num_scalar_prefetch=2,
        grid=(hidden // HIDDEN_BLOCK,),
        in_specs=[
            whole(tokens, features),
            whole(tokens, features),
            spec_we,
            pl.BlockSpec((per_step, rows_r, features), lambda i, *_: (i, 1, 0)),
            pl.BlockSpec((1, HIDDEN_BLOCK), lambda i, *_: (0, i)),
        ],
        out_specs=[
            whole(tokens, features),
            whole(tokens, features),
            whole(half, rows_r, features),
            whole(half, rows_r, features),
            *spec_e,
            pl.BlockSpec((1, HIDDEN_BLOCK), lambda i, *_: (0, i)),
        ],
        scratch_shapes=[
            pltpu.VMEM((tokens, HIDDEN_BLOCK), bf16),
            pltpu.VMEM((tokens, HIDDEN_BLOCK), bf16),
            pltpu.VMEM((features, HIDDEN_BLOCK), bf16),
        ],
    )
    y, da2, keep_r, send_r, keep_e, send_e, grad_b = pl.pallas_call(
        mlp_kernel,
        grid_spec=grid_spec,
        out_shape=[
            jax.ShapeDtypeStruct((tokens, features), f32),
            jax.ShapeDtypeStruct((tokens, features), f32),
            jax.ShapeDtypeStruct((half, rows_r, features), bf16),
            jax.ShapeDtypeStruct((half, rows_r, features), bf16),
            jax.ShapeDtypeStruct(shape_e[0], bf16),
            jax.ShapeDtypeStruct(shape_e[1], bf16),
            jax.ShapeDtypeStruct((1, hidden), f32),
        ],
        compiler_params=pltpu.CompilerParams(
            dimension_semantics=("arbitrary",), vmem_limit_bytes=56 << 20
        ),
        cost_estimate=pl.CostEstimate(
            flops=12 * tokens * features * hidden,
            transcendentals=2 * tokens * hidden,
            bytes_accessed=8 * features * hidden + 12 * tokens * features,
        ),
        name="mlp",
    )(block_places(order_r), block_places(order_e), a2, dy, we, both, bias[None])
    if not direct:
        keep_e, send_e = halves(by_place(keep_e.reshape(devices, rows_e, hidden), order_e))
    return y, da2, (keep_r, send_r), (keep_e, send_e), grad_b


def head_lanes(shape, head):
    lane = lax.broadcasted_iota(jnp.int32, shape, 1)
    return (lane >= head * HEAD_DIM) & (lane < (head + 1) * HEAD_DIM)


def scaled_scores(q, k, seg_col, seg_row):
    scores = dot(q, k, ((1,), (1,))) * HEAD_DIM ** (-0.5)
    return jnp.where(seg_col == seg_row, scores, -1e30)


def attend_kernel(q, k, v, seg_col, seg_row, out, out_lse):
    both_out, both_lse = [], []
    for head in range(2):
        mine = head_lanes(q.shape, head)
        q_head = jnp.where(mine, q[...].astype(f32), 0.0).astype(bf16)
        scores = scaled_scores(q_head, k[...], seg_col[...], seg_row[...])
        highest = jnp.max(scores, axis=-1, keepdims=True)
        weights = jnp.exp(scores - highest)
        total = jnp.sum(weights, axis=-1, keepdims=True)
        shares = (weights / total).astype(bf16)
        both_out.append(dot(shares, v[...]))
        both_lse.append(highest + jnp.log(total))
    first = head_lanes(q.shape, 0)
    out[...] = jnp.where(first, both_out[0], both_out[1]).astype(bf16)
    out_lse[...] = jnp.where(first, both_lse[0], both_lse[1])


def attend_back_kernel(q, k, v, d_out, lse, seg_col, seg_row, out_dq, out_dk, out_dv):
    parts = []
    for head in range(2):
        mine = head_lanes(q.shape, head)
        q_head = jnp.where(mine, q[...].astype(f32), 0.0).astype(bf16)
        d_head = jnp.where(mine, d_out[...].astype(f32), 0.0).astype(bf16)
        scores = scaled_scores(q_head, k[...], seg_col[...], seg_row[...])
        chances = jnp.exp(scores - lse[:, head * HEAD_DIM : head * HEAD_DIM + 1])
        d_chances = dot(d_head, v[...], ((1,), (1,)))
        row_dot = jnp.sum(chances * d_chances, axis=-1, keepdims=True)
        d_scores = (chances * (d_chances - row_dot)).astype(bf16)
        parts.append(
            (
                dot(d_scores, k[...]) * HEAD_DIM ** (-0.5),
                dot(d_scores, q[...], ((0,), (0,))) * HEAD_DIM ** (-0.5),
                dot(chances.astype(bf16), d_out[...], ((0,), (0,))),
            )
        )
    first = head_lanes(q.shape, 0)
    for ref, left, right in zip((out_dq, out_dk, out_dv), *parts):
        ref[...] = jnp.where(first, left, right).astype(bf16)


def attention(query_key, values, segments, extra=None):
    tokens, features = values.shape
    pairs = features // (2 * HEAD_DIM)
    head = pl.BlockSpec((tokens, 2 * HEAD_DIM), lambda i: (0, i))
    key = pl.BlockSpec((tokens, 2 * HEAD_DIM), lambda i: (0, i + pairs))
    whole = lambda *shape: pl.BlockSpec(shape, lambda i: (0,) * len(shape))
    segs = [segments[:, None], segments[None, :]]
    seg_specs = [whole(tokens, 1), whole(1, tokens)]
    shape = lambda kind: jax.ShapeDtypeStruct((tokens, features), kind)
    more = [] if extra is None else list(extra)
    outs = [shape(bf16), shape(f32)] if extra is None else [shape(bf16)] * 3
    products = 2 if extra is None else 5
    return pl.pallas_call(
        attend_kernel if extra is None else attend_back_kernel,
        grid=(pairs,),
        in_specs=[head, key, head] + [head] * len(more) + seg_specs,
        out_specs=[head] * len(outs),
        out_shape=outs,
        compiler_params=pltpu.CompilerParams(
            dimension_semantics=("arbitrary",), vmem_limit_bytes=48 << 20
        ),
        cost_estimate=pl.CostEstimate(
            flops=4 * products * tokens * tokens * features,
            transcendentals=2 * pairs * tokens * tokens,
            bytes_accessed=16 * tokens * features,
        ),
        name="attend" if extra is None else "attend_back",
    )(query_key, query_key, values, *more, *segs)


def on_device(
    grid_tokens,
    grid_cotangent,
    send_rows,
    send_counts,
    holder_segments,
    packed_master,
    packed_first,
    packed_second,
    mixing_master,
    mixing_first,
    mixing_second,
    expand_master,
    expand_first,
    expand_second,
    reduce_master,
    reduce_first,
    reduce_second,
    vector_master,
    vector_first,
    vector_second,
):
    devices = lax.axis_size(AXES)
    holding = send_rows.shape[1]
    slot_rows = holding // devices
    tokens, features = grid_tokens.shape
    first, second = bit_orders()
    segments = holder_segments[0]

    slots = jnp.arange(slot_rows, dtype=jnp.int32)[None, :]
    live = (slots < send_counts[0][:, None]).reshape(holding)
    row_index = jnp.where(live, send_rows[0], -1)
    pick = (row_index[:, None] == jnp.arange(tokens, dtype=jnp.int32)[None, :]).astype(bf16)

    def send(rows):
        blocks = rows.reshape(devices, slot_rows, features)
        moved = lax.all_to_all(blocks, AXES, split_axis=0, concat_axis=0, tiled=True)
        return moved.reshape(holding, features)

    def put_rows(rows):
        return dot(pick, rows, ((0,), (0,))).astype(bf16)

    low = packed_master.astype(bf16)
    cut = 2 * features
    lines = vector_master.shape[0]
    padded = jnp.pad(vector_master.T.astype(bf16), ((0, 0), (0, 128 - lines)))
    late = jnp.concatenate([low[:, cut:], mixing_master.astype(bf16), padded], axis=1)
    gathers = [Gather(low[:, :cut], first), Gather(late, second)]
    rows_e, hidden = expand_master.shape
    tall = expand_master.astype(bf16).reshape(rows_e, hidden // features, features)
    tall = tall.transpose(1, 0, 2).reshape(-1, features)
    tall = jnp.concatenate([tall, reduce_master.astype(bf16)], axis=0)
    w_mlp = lax.all_gather(tall, AXES, axis=0, tiled=False)

    picked = dot(pick, grid_tokens).astype(bf16)
    picked_grad = dot(pick, grid_cotangent).astype(bf16)
    low_stages = lax.axis_size("col").bit_length() - 2
    while gathers[0].left:
        stage = len(first) - len(gathers[0].left)
        if stage == low_stages:
            picked = gather_turn(picked, gathers)
            arrived = send(picked)
        elif len(gathers[0].left) == 1:
            picked_grad = gather_turn(picked_grad, gathers)
            arrived_grad = send(picked_grad)
        else:
            gather_turn((), gathers)
    early = gathers[0].blocks().reshape(features, cut)
    late = gathers[1].blocks().reshape(features, 2 * features + 128)
    w_value, w_mixing = late[:, :features], late[:, features : 2 * features]
    vectors = late[:, 2 * features : 2 * features + lines].T.astype(f32)
    gain_one, shift_one, bias_query, bias_value, bias_mixing = (vectors[i] for i in range(5))
    gain_two, shift_two, bias_output = (vectors[i] for i in range(5, 8))
    bias_hidden = vectors[8:].reshape(-1)

    inputs = arrived.astype(f32)
    normed_one, factor_one = normalize(inputs)
    layer_one = (normed_one * gain_one + shift_one).astype(bf16)
    joined_bias = jnp.concatenate([bias_query, jnp.zeros_like(bias_query)])
    query_key = (dot(layer_one, early) + joined_bias).astype(bf16)
    values = (dot(layer_one, w_value) + bias_value).astype(bf16)
    attended, log_total = attention(query_key, values, segments)
    middle = inputs + dot(attended, w_mixing) + bias_mixing
    normed_two, factor_two = normalize(middle)
    layer_two = (normed_two * gain_two + shift_two).astype(bf16)
    branch, d_layer_two, grad_reduce, grad_expand, grad_hidden = mlp(
        layer_two, arrived_grad, w_mlp, bias_hidden, first, second
    )
    chain_reduce = Chain(*grad_reduce, first)
    chain_expand = Chain(*grad_expand, second)
    chains = [chain_reduce, chain_expand]
    outputs = (middle + branch + bias_output).astype(bf16)

    upstream = arrived_grad.astype(f32)
    d_middle = upstream + norm_back(d_layer_two, normed_two, factor_two, gain_two)
    d_branch = d_middle.astype(bf16)
    d_attended = dot(d_branch, w_mixing, ((1,), (1,))).astype(bf16)
    early_reads = (d_attended, outputs, layer_one, attended, d_branch, d_layer_two, normed_two, upstream)
    early_reads = turn(early_reads, chains)
    d_attended, outputs, layer_one, attended, d_branch, d_layer_two, normed_two, upstream = early_reads
    moved = send(outputs)
    d_query, d_key, d_value = attention(query_key, values, segments, (d_attended, log_total))
    chain_late = weight_chain([(layer_one, d_value), (attended, d_branch)], first)
    chain_query_key = weight_chain([(layer_one, d_query), (layer_one, d_key)], second)
    chains += [chain_late, chain_query_key]
    d_query_key = jnp.concatenate([d_query, d_key], axis=1)
    d_layer_one = dot(d_query_key, early, ((1,), (1,))) + dot(d_value, w_value, ((1,), (1,)))
    input_grads = d_middle + norm_back(d_layer_one, normed_one, factor_one, gain_one)
    input_grads = input_grads.astype(bf16)
    total = lambda part: jnp.sum(part.astype(f32), axis=0, keepdims=True)
    grad_vector = jnp.concatenate(
        [
            total(d_layer_one * normed_one),
            total(d_layer_one),
            total(d_query),
            total(d_value),
            total(d_branch),
            total(d_layer_two * normed_two),
            total(d_layer_two),
            total(upstream),
            grad_hidden.reshape(-1, features),
        ],
        axis=0,
    )
    vector_blocks = grad_vector.T.reshape(devices, -1, lines)
    vector_blocks = by_place(vector_blocks, second)
    input_grads, vector_blocks, moved = turn((input_grads, vector_blocks, moved), chains)
    moved_grad = send(input_grads)
    chain_vector = Chain(*halves(vector_blocks), second, f32)
    chains.append(chain_vector)
    moved = turn(moved, chains)
    grid_output = put_rows(moved)
    moved_grad = turn(moved_grad, chains)
    input_gradient = put_rows(moved_grad)
    while any(chain.order for chain in chains):
        turn((), [chain for chain in chains if chain.order])
    masters = (packed_master, mixing_master, expand_master, reduce_master, vector_master)
    firsts = (packed_first, mixing_first, expand_first, reduce_first, vector_first)
    seconds = (packed_second, mixing_second, expand_second, reduce_second, vector_second)
    late_sum = chain_late.total()
    shares = (
        jnp.concatenate([chain_query_key.total(), late_sum[:, :features]], axis=1),
        late_sum[:, features:],
        chain_expand.total(),
        chain_reduce.total(),
        chain_vector.total().T,
    )
    updates = [
        adamw(
            masters[number],
            firsts[number],
            seconds[number],
            shares[number],
            weight_rates[number],
            decay_rates[number],
        )
        for number in range(5)
    ]
    return (
        grid_output,
        input_gradient,
        updates[0][0],
        updates[0][1],
        updates[0][2],
        updates[1][0],
        updates[1][1],
        updates[1][2],
        updates[2][0],
        updates[2][1],
        updates[2][2],
        updates[3][0],
        updates[3][1],
        updates[3][2],
        updates[4][0],
        updates[4][1],
        updates[4][2],
    )


def solution(mesh):
    in_specs = (
        P(("row", "col"), None),
        P(("row", "col"), None),
        P(("row", "col"), None),
        P(("row", "col"), None),
        P(("row", "col"), None),
        P(("row", "col"), None),
        P(("row", "col"), None),
        P(("row", "col"), None),
        P(("row", "col"), None),
        P(("row", "col"), None),
        P(("row", "col"), None),
        P(("row", "col"), None),
        P(("row", "col"), None),
        P(("row", "col"), None),
        P(("row", "col"), None),
        P(("row", "col"), None),
        P(("row", "col"), None),
        P(None, ("row", "col")),
        P(None, ("row", "col")),
        P(None, ("row", "col")),
    )
    out_specs = (
        P(("row", "col"), None),
        P(("row", "col"), None),
        P(("row", "col"), None),
        P(("row", "col"), None),
        P(("row", "col"), None),
        P(("row", "col"), None),
        P(("row", "col"), None),
        P(("row", "col"), None),
        P(("row", "col"), None),
        P(("row", "col"), None),
        P(("row", "col"), None),
        P(("row", "col"), None),
        P(("row", "col"), None),
        P(("row", "col"), None),
        P(None, ("row", "col")),
        P(None, ("row", "col")),
        P(None, ("row", "col")),
    )
    return jax.shard_map(
        on_device, mesh=mesh, in_specs=in_specs, out_specs=out_specs, check_vma=False
    )
```

```python
import jax
import jax.numpy as jnp
from jax import lax
from jax.experimental import pallas as pl
from jax.experimental.pallas import tpu as pltpu
from jax.sharding import PartitionSpec as P

HEAD_DIM = 64


weight_rates = (0.07, 0.55, 0.07, 0.036, 0.4)
decay_rates = (0.05, 0.05, 0.05, 0.05, 0.0)


def normalize(values):
    center = values - jnp.mean(values, axis=-1, keepdims=True)
    spread = jnp.mean(center * center, axis=-1, keepdims=True)
    factor = lax.rsqrt(spread + 1e-06)
    return (center * factor, factor)


def norm_back(upstream, normed, factor, gain):
    scaled = upstream * gain
    return factor * (
        scaled
        - jnp.mean(scaled, axis=-1, keepdims=True)
        - normed * jnp.mean(scaled * normed, axis=-1, keepdims=True)
    )


def adamw(master, moment_one, moment_two, gradient, step_rate, decay_rate):
    first_new = 0.9 * moment_one + 0.1 * gradient
    second_new = 0.95 * moment_two + 0.05 * gradient * gradient
    moved = first_new / (1.0 - 0.9**10) / (jnp.sqrt(second_new / (1.0 - 0.95**10)) + 1e-08)
    return (master - step_rate * (moved + decay_rate * master), first_new, second_new)


AXES = ("row", "col")
HIDDEN_BLOCK = 768
TOKEN_BLOCK = 256
f32 = jnp.float32
bf16 = jnp.bfloat16


def dot(left, right, dims=((1,), (0,))):
    return lax.dot_general(left, right, (dims, ((), ())), preferred_element_type=f32)


def swap(values, bit):
    devices = lax.axis_size(AXES)
    return lax.ppermute(values, AXES, [(d, d ^ (1 << bit)) for d in range(devices)])


def bit_orders():
    rows, cols = lax.axis_size("row"), lax.axis_size("col")
    low_bits = cols.bit_length() - 1
    all_bits = (rows * cols).bit_length() - 1
    core, high, low = low_bits, list(range(low_bits + 1, all_bits)), list(range(low_bits))
    return ([core] + high + low, [core] + low[:1] + high + low[1:])


def place_of(order):
    count = len(order)
    return [
        sum(((r >> bit) & 1) << (count - 1 - step) for step, bit in enumerate(order))
        for r in range(1 << count)
    ]


def block_places(order):
    table = jnp.asarray(place_of(order), jnp.int32)
    ranks = jnp.arange(len(table), dtype=jnp.int32) ^ lax.axis_index(AXES)
    return jnp.take(table, ranks, mode="clip")


def by_place(blocks, order):
    table = place_of(order)
    back = [table.index(p) for p in range(len(table))]
    ranks = jnp.asarray(back, jnp.int32) ^ lax.axis_index(AXES)
    return jnp.take(blocks, ranks, axis=0, mode="clip")


class Chain:
    def __init__(self, keep, send, order):
        self.keep, self.send, self.order = keep, send, list(order)
        self.launch()

    def launch(self):
        self.got = swap(self.send, self.order.pop(0))

    def merge(self):
        half = self.keep.shape[0] // 2
        keep, got = self.keep, self.got
        self.send = keep[half:] + got[half:]
        self.keep = keep[:half] + got[:half]

    def total(self):
        return (self.keep.astype(f32) + self.got.astype(f32))[0]


def turn(values, chains):
    values, gots = lax.optimization_barrier((values, [c.got for c in chains]))
    for chain, got in zip(chains, gots):
        chain.got = got
        chain.merge()
    values, sends = lax.optimization_barrier((values, [c.send for c in chains]))
    for chain, part in zip(chains, sends):
        chain.send = part
        chain.launch()
    return values


def halves(blocks):
    half = blocks.shape[0] // 2
    return blocks[:half], blocks[half:]


def weight_chain(pairs, order):
    devices = lax.axis_size(AXES)
    keeps, sends = [], []
    for left, right in pairs:
        tokens, features = left.shape
        rows = features // devices
        turned = by_place(left.T.reshape(devices, rows, tokens), order)
        for side, parts in zip(halves(turned), (keeps, sends)):
            flat = dot(side.reshape(-1, tokens), right).astype(bf16)
            parts.append(flat.reshape(-1, rows, right.shape[1]))
    join = lambda parts: parts[0] if len(parts) == 1 else jnp.concatenate(parts, axis=-1)
    return Chain(join(keeps), join(sends), order)


class Gather:
    def __init__(self, shard, order):
        self.order, self.held, self.left = order, shard[None], list(reversed(order))
        self.launch()

    def launch(self):
        self.got = swap(self.held, self.left.pop(0))

    def merge(self):
        self.held = jnp.concatenate([self.held, self.got], axis=0)

    def blocks(self):
        self.merge()
        return jnp.take(self.held, block_places(self.order), axis=0, mode="clip")


def gather_turn(values, gathers):
    values, gots = lax.optimization_barrier((values, [g.got for g in gathers]))
    for gather, got in zip(gathers, gots):
        gather.got = got
        gather.merge()
    values, helds = lax.optimization_barrier((values, [g.held for g in gathers]))
    for gather, held in zip(gathers, helds):
        gather.held = held
        gather.launch()
    return values


def store_by_place(place, block, keep, send):
    half = keep.shape[0]

    @pl.when(place < half)
    def _():
        keep[place] = block

    @pl.when(place >= half)
    def _():
        send[place - half] = block


def mlp_kernel(
    place_r, place_e, a2, dy, we, wr, bias,
    out_y, out_da, keep_r, send_r, keep_e, send_e, out_gb, u_all, dz_all, we_all,
):
    step = pl.program_id(0)
    tokens, features = a2.shape
    half = keep_r.shape[0]

    @pl.when(step == 0)
    def _():
        out_y[...] = jnp.zeros_like(out_y)
        out_da[...] = jnp.zeros_like(out_da)

    if len(we.shape) == 2:
        we_all[...] = we[...]
    else:
        rows_e = we.shape[1]
        for s in range(we.shape[0]):
            we_all[s * rows_e : (s + 1) * rows_e, :] = we[s]
    wr_all = wr[...].reshape(HIDDEN_BLOCK, features)

    def chunk(number, total):
        rows = pl.ds(pl.multiple_of(number * TOKEN_BLOCK, TOKEN_BLOCK), TOKEN_BLOCK)
        z = dot(a2[rows, :], we_all[...]) + bias[...]
        cumulative = 0.5 * (1.0 + lax.erf(z * 0.7071067811865476))
        u = (z * cumulative).astype(bf16)
        slope = cumulative + z * jnp.exp(-0.5 * z * z) * 0.3989422804014327
        dz = (dot(dy[rows, :], wr_all, ((1,), (1,))) * slope).astype(bf16)
        u_all[rows, :] = u
        dz_all[rows, :] = dz
        out_y[rows, :] += dot(u, wr_all)
        out_da[rows, :] += dot(dz, we_all[...], ((1,), (1,)))
        return total + jnp.sum(dz.astype(f32), axis=0, keepdims=True)

    out_gb[...] = lax.fori_loop(0, tokens // TOKEN_BLOCK, chunk, jnp.zeros(out_gb.shape, f32))

    rows_r = keep_r.shape[1]
    per_step = HIDDEN_BLOCK // rows_r
    grad = dot(u_all[...], dy[...], ((0,), (0,))).astype(bf16)
    for j in range(per_step):
        store_by_place(place_r[step * per_step + j], grad[j * rows_r : (j + 1) * rows_r], keep_r, send_r)
    grad = dot(a2[...], dz_all[...], ((0,), (0,))).astype(bf16)
    if len(keep_e.shape) == 2:
        keep_e[...] = grad
    else:
        rows_e = keep_e.shape[1]
        for s in range(2 * half):
            store_by_place(place_e[s], grad[s * rows_e : (s + 1) * rows_e], keep_e, send_e)


def mlp(a2, dy, both, bias, order_r, order_e):
    devices = lax.axis_size(AXES)
    tokens, features = a2.shape
    rows_r = both.shape[1] // 2
    hidden = devices * rows_r
    rows_e, wide = features // devices, hidden // features
    half = devices // 2
    direct = rows_e % 8 == 0
    whole = lambda *shape: pl.BlockSpec(shape, lambda i, *_: (0,) * len(shape))
    columns = pl.BlockSpec((features, HIDDEN_BLOCK), lambda i, *_: (0, i))
    if direct:
        we = both.reshape(devices, 2 * wide, rows_e, features)
        spec_we = pl.BlockSpec((devices, None, rows_e, features), lambda i, *_: (0, i, 0, 0))
        spec_e = [pl.BlockSpec((half, rows_e, HIDDEN_BLOCK), lambda i, *_: (0, 0, i))] * 2
        shape_e = [(half, rows_e, hidden)] * 2
    else:
        we = both[:, :rows_r].reshape(devices, wide, rows_e, features)
        we = we.transpose(0, 2, 1, 3).reshape(features, hidden)
        spec_we = columns
        spec_e = [columns, pl.BlockSpec((8, HIDDEN_BLOCK), lambda i, *_: (0, i))]
        shape_e = [(features, hidden), (8, hidden)]
    per_step = HIDDEN_BLOCK // rows_r
    grid_spec = pltpu.PrefetchScalarGridSpec(
        num_scalar_prefetch=2,
        grid=(hidden // HIDDEN_BLOCK,),
        in_specs=[
            whole(tokens, features),
            whole(tokens, features),
            spec_we,
            pl.BlockSpec((per_step, rows_r, features), lambda i, *_: (i, 1, 0)),
            pl.BlockSpec((1, HIDDEN_BLOCK), lambda i, *_: (0, i)),
        ],
        out_specs=[
            whole(tokens, features),
            whole(tokens, features),
            whole(half, rows_r, features),
            whole(half, rows_r, features),
            *spec_e,
            pl.BlockSpec((1, HIDDEN_BLOCK), lambda i, *_: (0, i)),
        ],
        scratch_shapes=[
            pltpu.VMEM((tokens, HIDDEN_BLOCK), bf16),
            pltpu.VMEM((tokens, HIDDEN_BLOCK), bf16),
            pltpu.VMEM((features, HIDDEN_BLOCK), bf16),
        ],
    )
    y, da2, keep_r, send_r, keep_e, send_e, grad_b = pl.pallas_call(
        mlp_kernel,
        grid_spec=grid_spec,
        out_shape=[
            jax.ShapeDtypeStruct((tokens, features), f32),
            jax.ShapeDtypeStruct((tokens, features), f32),
            jax.ShapeDtypeStruct((half, rows_r, features), bf16),
            jax.ShapeDtypeStruct((half, rows_r, features), bf16),
            jax.ShapeDtypeStruct(shape_e[0], bf16),
            jax.ShapeDtypeStruct(shape_e[1], bf16),
            jax.ShapeDtypeStruct((1, hidden), f32),
        ],
        compiler_params=pltpu.CompilerParams(
            dimension_semantics=("arbitrary",), vmem_limit_bytes=56 << 20
        ),
        cost_estimate=pl.CostEstimate(
            flops=12 * tokens * features * hidden,
            transcendentals=2 * tokens * hidden,
            bytes_accessed=8 * features * hidden + 12 * tokens * features,
        ),
        name="mlp",
    )(block_places(order_r), block_places(order_e), a2, dy, we, both, bias[None])
    if not direct:
        keep_e, send_e = halves(by_place(keep_e.reshape(devices, rows_e, hidden), order_e))
    return y, da2, (keep_r, send_r), (keep_e, send_e), grad_b


def head_lanes(shape, head):
    lane = lax.broadcasted_iota(jnp.int32, shape, 1)
    return (lane >= head * HEAD_DIM) & (lane < (head + 1) * HEAD_DIM)


def scaled_scores(q, k, seg_col, seg_row):
    scores = dot(q, k, ((1,), (1,))) * HEAD_DIM ** (-0.5)
    return jnp.where(seg_col == seg_row, scores, -1e30)


def attend_kernel(q, k, v, seg_col, seg_row, out, out_lse):
    both_out, both_lse = [], []
    for head in range(2):
        mine = head_lanes(q.shape, head)
        q_head = jnp.where(mine, q[...].astype(f32), 0.0).astype(bf16)
        scores = scaled_scores(q_head, k[...], seg_col[...], seg_row[...])
        highest = jnp.max(scores, axis=-1, keepdims=True)
        weights = jnp.exp(scores - highest)
        total = jnp.sum(weights, axis=-1, keepdims=True)
        shares = (weights / total).astype(bf16)
        both_out.append(dot(shares, v[...]))
        both_lse.append(highest + jnp.log(total))
    first = head_lanes(q.shape, 0)
    out[...] = jnp.where(first, both_out[0], both_out[1]).astype(bf16)
    out_lse[...] = jnp.where(first, both_lse[0], both_lse[1])


def attend_back_kernel(q, k, v, d_out, lse, seg_col, seg_row, out):
    parts = []
    for head in range(2):
        mine = head_lanes(q.shape, head)
        q_head = jnp.where(mine, q[...].astype(f32), 0.0).astype(bf16)
        d_head = jnp.where(mine, d_out[...].astype(f32), 0.0).astype(bf16)
        scores = scaled_scores(q_head, k[...], seg_col[...], seg_row[...])
        chances = jnp.exp(scores - lse[:, head * HEAD_DIM : head * HEAD_DIM + 1])
        d_chances = dot(d_head, v[...], ((1,), (1,)))
        row_dot = jnp.sum(chances * d_chances, axis=-1, keepdims=True)
        d_scores = (chances * (d_chances - row_dot)).astype(bf16)
        parts.append(
            (
                dot(d_scores, k[...]) * HEAD_DIM ** (-0.5),
                dot(d_scores, q[...], ((0,), (0,))) * HEAD_DIM ** (-0.5),
                dot(chances.astype(bf16), d_out[...], ((0,), (0,))),
            )
        )
    first = head_lanes(q.shape, 0)
    for number, (left, right) in enumerate(zip(*parts)):
        out[number] = jnp.where(first, left, right).astype(bf16)


def attention(query_key, values, segments, extra=None):
    tokens, features = values.shape
    pairs = features // (2 * HEAD_DIM)
    head = pl.BlockSpec((tokens, 2 * HEAD_DIM), lambda i: (0, i))
    key = pl.BlockSpec((tokens, 2 * HEAD_DIM), lambda i: (0, i + pairs))
    whole = lambda *shape: pl.BlockSpec(shape, lambda i: (0,) * len(shape))
    segs = [segments[:, None], segments[None, :]]
    seg_specs = [whole(tokens, 1), whole(1, tokens)]
    shape = lambda kind: jax.ShapeDtypeStruct((tokens, features), kind)
    more = [] if extra is None else list(extra)
    if extra is None:
        outs, out_specs = [shape(bf16), shape(f32)], [head, head]
    else:
        outs = jax.ShapeDtypeStruct((3, tokens, features), bf16)
        out_specs = pl.BlockSpec((3, tokens, 2 * HEAD_DIM), lambda i: (0, 0, i))
    products = 2 if extra is None else 5
    return pl.pallas_call(
        attend_kernel if extra is None else attend_back_kernel,
        grid=(pairs,),
        in_specs=[head, key, head] + [head] * len(more) + seg_specs,
        out_specs=out_specs,
        out_shape=outs,
        compiler_params=pltpu.CompilerParams(
            dimension_semantics=("arbitrary",), vmem_limit_bytes=48 << 20
        ),
        cost_estimate=pl.CostEstimate(
            flops=4 * products * tokens * tokens * features,
            transcendentals=2 * pairs * tokens * tokens,
            bytes_accessed=16 * tokens * features,
        ),
        name="attend" if extra is None else "attend_back",
    )(query_key, query_key, values, *more, *segs)


def sums_of(*parts):
    rows = [jnp.sum(part.astype(f32), axis=0, keepdims=True) for part in parts]
    return jnp.concatenate(rows + [jnp.zeros_like(rows[0])] * (8 - len(rows)), axis=0)


def middle_kernel(middle, branch, d_two, dy, gain, bias, wm, y, d_middle, d_branch, d_out, sums):
    normed, factor = normalize(middle[...])
    y[...] = (middle[...] + branch[...] + bias[...]).astype(bf16)
    upstream = dy[...].astype(f32)
    grad = upstream + norm_back(d_two[...], normed, factor, gain[...])
    low = grad.astype(bf16)
    d_middle[...] = grad
    d_branch[...] = low
    d_out[...] = dot(low, wm[...], ((1,), (1,))).astype(bf16)

    @pl.when(pl.program_id(0) == 0)
    def _():
        sums[...] = jnp.zeros_like(sums)

    sums[...] += sums_of(low, d_two[...] * normed, d_two[...], upstream)


def first_kernel(grads, w_qk, w_v, x, d_middle, gain, dx, sums):
    features = x.shape[1]
    d_one = dot(grads[0], w_qk[:, :features], ((1,), (1,)))
    d_one += dot(grads[1], w_qk[:, features:], ((1,), (1,)))
    d_one += dot(grads[2], w_v[...], ((1,), (1,)))
    normed, factor = normalize(x[...].astype(f32))
    dx[...] = (d_middle[...] + norm_back(d_one, normed, factor, gain[...])).astype(bf16)

    @pl.when(pl.program_id(0) == 0)
    def _():
        sums[...] = jnp.zeros_like(sums)

    sums[...] += sums_of(d_one * normed, d_one, grads[0], grads[2])


def by_rows(kernel, tokens, operands, out_kinds, flops):
    features = operands[0].shape[-1]

    def spec(shape):
        if len(shape) > 1 and shape[-2] == tokens:
            lead = len(shape) - 2
            return pl.BlockSpec(
                shape[:-2] + (TOKEN_BLOCK, shape[-1]), lambda i: (0,) * lead + (i, 0)
            )
        return pl.BlockSpec(shape, lambda i: (0,) * len(shape))

    outs = [jax.ShapeDtypeStruct((tokens, features), kind) for kind in out_kinds]
    outs.append(jax.ShapeDtypeStruct((8, features), f32))
    return pl.pallas_call(
        kernel,
        grid=(tokens // TOKEN_BLOCK,),
        in_specs=[spec(x.shape) for x in operands],
        out_specs=[spec(x.shape) for x in outs],
        out_shape=outs,
        compiler_params=pltpu.CompilerParams(
            dimension_semantics=("arbitrary",), vmem_limit_bytes=48 << 20
        ),
        cost_estimate=pl.CostEstimate(
            flops=flops,
            transcendentals=0,
            bytes_accessed=sum(x.size * x.dtype.itemsize for x in [*operands, *outs]),
        ),
    )(*operands)


def products_kernel(place_qk, place_vm, a1, o, grads, dbr, keep_qk, send_qk, keep_vm, send_vm):
    step = pl.program_id(0)
    last = step == 3
    left = jnp.where(last, o[...].astype(f32), a1[...].astype(f32)).astype(bf16)
    right = jnp.where(last, dbr[...].astype(f32), grads[...].astype(f32)).astype(bf16)
    out = dot(left, right, ((0,), (0,))).astype(bf16)
    half, rows = keep_qk.shape[:2]

    @pl.when(step < 2)
    def _():
        for s in range(2 * half):
            store_by_place(place_qk[s], out[s * rows : (s + 1) * rows], keep_qk, send_qk)

    @pl.when(step >= 2)
    def _():
        for s in range(2 * half):
            store_by_place(place_vm[s], out[s * rows : (s + 1) * rows], keep_vm, send_vm)


def product_chains(a1, o, grads, dbr, order_qk, order_vm):
    devices = lax.axis_size(AXES)
    tokens, features = a1.shape
    rows, half = features // devices, devices // 2
    if rows % 8:
        return (
            weight_chain([(a1, grads[0]), (a1, grads[1])], order_qk),
            weight_chain([(a1, grads[2]), (o, dbr)], order_vm),
        )
    whole = pl.BlockSpec((tokens, features), lambda i, *_: (0, 0))
    spec_qk = pl.BlockSpec((half, rows, features), lambda i, *_: (0, 0, jnp.minimum(i, 1)))
    spec_vm = pl.BlockSpec((half, rows, features), lambda i, *_: (0, 0, jnp.maximum(i - 2, 0)))
    third = pl.BlockSpec((None, tokens, features), lambda i, *_: (jnp.minimum(i, 2), 0, 0))
    keep_qk, send_qk, keep_vm, send_vm = pl.pallas_call(
        products_kernel,
        grid_spec=pltpu.PrefetchScalarGridSpec(
            num_scalar_prefetch=2,
            grid=(4,),
            in_specs=[whole, whole, third, whole],
            out_specs=[spec_qk, spec_qk, spec_vm, spec_vm],
        ),
        out_shape=[jax.ShapeDtypeStruct((half, rows, 2 * features), bf16)] * 4,
        compiler_params=pltpu.CompilerParams(
            dimension_semantics=("arbitrary",), vmem_limit_bytes=48 << 20
        ),
        cost_estimate=pl.CostEstimate(
            flops=8 * tokens * features * features,
            transcendentals=0,
            bytes_accessed=12 * tokens * features + 8 * features * features,
        ),
        name="products",
    )(block_places(order_qk), block_places(order_vm), a1, o, grads, dbr)
    return Chain(keep_qk, send_qk, order_qk), Chain(keep_vm, send_vm, order_vm)


def on_device(
    grid_tokens,
    grid_cotangent,
    send_rows,
    send_counts,
    holder_segments,
    packed_master,
    packed_first,
    packed_second,
    mixing_master,
    mixing_first,
    mixing_second,
    expand_master,
    expand_first,
    expand_second,
    reduce_master,
    reduce_first,
    reduce_second,
    vector_master,
    vector_first,
    vector_second,
):
    devices = lax.axis_size(AXES)
    holding = send_rows.shape[1]
    slot_rows = holding // devices
    tokens, features = grid_tokens.shape
    first, second = bit_orders()
    segments = holder_segments[0]

    slots = jnp.arange(slot_rows, dtype=jnp.int32)[None, :]
    live = (slots < send_counts[0][:, None]).reshape(holding)
    row_index = jnp.where(live, send_rows[0], -1)
    pick = (row_index[:, None] == jnp.arange(tokens, dtype=jnp.int32)[None, :]).astype(bf16)

    def send(rows):
        blocks = rows.reshape(devices, slot_rows, features)
        moved = lax.all_to_all(blocks, AXES, split_axis=0, concat_axis=0, tiled=True)
        return moved.reshape(holding, features)

    def put_rows(rows):
        return dot(pick, rows, ((0,), (0,))).astype(bf16)

    low = packed_master.astype(bf16)
    cut = 2 * features
    lines = vector_master.shape[0]
    padded = jnp.pad(vector_master.T.astype(bf16), ((0, 0), (0, 128 - lines)))
    late = jnp.concatenate([low[:, cut:], mixing_master.astype(bf16), padded], axis=1)
    gathers = [Gather(low[:, :cut], first), Gather(late, second)]
    rows_e, hidden = expand_master.shape
    tall = expand_master.astype(bf16).reshape(rows_e, hidden // features, features)
    tall = tall.transpose(1, 0, 2).reshape(-1, features)
    tall = jnp.concatenate([tall, reduce_master.astype(bf16)], axis=0)
    w_mlp = lax.all_gather(tall, AXES, axis=0, tiled=False)

    picked = dot(pick, grid_tokens).astype(bf16)
    picked_grad = dot(pick, grid_cotangent).astype(bf16)
    low_stages = lax.axis_size("col").bit_length() - 2
    while gathers[0].left:
        stage = len(first) - len(gathers[0].left)
        if stage == low_stages:
            picked = gather_turn(picked, gathers)
            arrived = send(picked)
        elif len(gathers[0].left) == 1:
            picked_grad = gather_turn(picked_grad, gathers)
            arrived_grad = send(picked_grad)
        else:
            gather_turn((), gathers)
    early = gathers[0].blocks().reshape(features, cut)
    late = gathers[1].blocks().reshape(features, 2 * features + 128)
    w_value, w_mixing = late[:, :features], late[:, features : 2 * features]
    vectors = late[:, 2 * features : 2 * features + lines].T.astype(f32)
    gain_one, shift_one, bias_query, bias_value, bias_mixing = (vectors[i] for i in range(5))
    gain_two, shift_two, bias_output = (vectors[i] for i in range(5, 8))
    bias_hidden = vectors[8:].reshape(-1)

    inputs = arrived.astype(f32)
    normed_one, _ = normalize(inputs)
    layer_one = (normed_one * gain_one + shift_one).astype(bf16)
    joined_bias = jnp.concatenate([bias_query, jnp.zeros_like(bias_query)])
    query_key = (dot(layer_one, early) + joined_bias).astype(bf16)
    values = (dot(layer_one, w_value) + bias_value).astype(bf16)
    attended, log_total = attention(query_key, values, segments)
    middle = inputs + dot(attended, w_mixing) + bias_mixing
    normed_two, _ = normalize(middle)
    layer_two = (normed_two * gain_two + shift_two).astype(bf16)
    branch, d_layer_two, grad_reduce, grad_expand, grad_hidden = mlp(
        layer_two, arrived_grad, w_mlp, bias_hidden, first, second
    )
    chain_reduce = Chain(*grad_reduce, first)
    chain_expand = Chain(*grad_expand, second)
    chains = [chain_reduce, chain_expand]

    outputs, d_middle, d_branch, d_attended, sums_two = by_rows(
        middle_kernel,
        holding,
        [middle, branch, d_layer_two, arrived_grad, gain_two[None], bias_output[None], w_mixing],
        [bf16, f32, bf16, bf16],
        2 * holding * features * features,
    )
    d_attended, outputs = turn((d_attended, outputs), chains)
    moved = send(outputs)
    grads = attention(query_key, values, segments, (d_attended, log_total))
    chains += product_chains(layer_one, attended, grads, d_branch, second, first)
    chain_query_key, chain_late = chains[2:]
    input_grads, sums_one = by_rows(
        first_kernel,
        holding,
        [grads, early, w_value, arrived, d_middle, gain_one[None]],
        [bf16],
        6 * holding * features * features,
    )
    grad_vector = jnp.concatenate(
        [sums_one[:4], sums_two[:4], grad_hidden.reshape(-1, features)], axis=0
    )
    vector_blocks = grad_vector.T.reshape(devices, -1, lines)
    vector_blocks = by_place(vector_blocks, second)
    input_grads, vector_blocks, moved = turn((input_grads, vector_blocks, moved), chains)
    moved_grad = send(input_grads)
    chain_vector = Chain(*halves(vector_blocks), second)
    chains.append(chain_vector)
    moved = turn(moved, chains)
    grid_output = put_rows(moved)
    moved_grad = turn(moved_grad, chains)
    input_gradient = put_rows(moved_grad)
    while any(chain.order for chain in chains):
        turn((), [chain for chain in chains if chain.order])
    masters = (packed_master, mixing_master, expand_master, reduce_master, vector_master)
    firsts = (packed_first, mixing_first, expand_first, reduce_first, vector_first)
    seconds = (packed_second, mixing_second, expand_second, reduce_second, vector_second)
    late_sum = chain_late.total()
    shares = (
        jnp.concatenate([chain_query_key.total(), late_sum[:, :features]], axis=1),
        late_sum[:, features:],
        chain_expand.total(),
        chain_reduce.total(),
        chain_vector.total().T,
    )
    updates = [
        adamw(
            masters[number],
            firsts[number],
            seconds[number],
            shares[number],
            weight_rates[number],
            decay_rates[number],
        )
        for number in range(5)
    ]
    return (
        grid_output,
        input_gradient,
        updates[0][0],
        updates[0][1],
        updates[0][2],
        updates[1][0],
        updates[1][1],
        updates[1][2],
        updates[2][0],
        updates[2][1],
        updates[2][2],
        updates[3][0],
        updates[3][1],
        updates[3][2],
        updates[4][0],
        updates[4][1],
        updates[4][2],
    )


def solution(mesh):
    in_specs = (
        P(("row", "col"), None),
        P(("row", "col"), None),
        P(("row", "col"), None),
        P(("row", "col"), None),
        P(("row", "col"), None),
        P(("row", "col"), None),
        P(("row", "col"), None),
        P(("row", "col"), None),
        P(("row", "col"), None),
        P(("row", "col"), None),
        P(("row", "col"), None),
        P(("row", "col"), None),
        P(("row", "col"), None),
        P(("row", "col"), None),
        P(("row", "col"), None),
        P(("row", "col"), None),
        P(("row", "col"), None),
        P(None, ("row", "col")),
        P(None, ("row", "col")),
        P(None, ("row", "col")),
    )
    out_specs = (
        P(("row", "col"), None),
        P(("row", "col"), None),
        P(("row", "col"), None),
        P(("row", "col"), None),
        P(("row", "col"), None),
        P(("row", "col"), None),
        P(("row", "col"), None),
        P(("row", "col"), None),
        P(("row", "col"), None),
        P(("row", "col"), None),
        P(("row", "col"), None),
        P(("row", "col"), None),
        P(("row", "col"), None),
        P(("row", "col"), None),
        P(None, ("row", "col")),
        P(None, ("row", "col")),
        P(None, ("row", "col")),
    )
    return jax.shard_map(
        on_device, mesh=mesh, in_specs=in_specs, out_specs=out_specs, check_vma=False
    )
```
